32 devices in a mesh: row: 8 (over z, y), col: 4 (over x, core).
Axes of the slice: x: 2, y: 2, z: 4, core: 2. Of those that a mesh axis runs over, the one named last changes fastest.
Arguments:
- tile_values: bfloat16 [128, 8, 256, 256], P(('row', 'col')), may hold values from -0.375 to 0.375
- block_columns: int32 [128, 8], P(('row', 'col')), may hold values from 0 to 127, as said below
- tile_counts: int32 [128], P(('row', 'col')), may hold values from 1 to 8, as said below
- diagonal: float32 [32768], P(('row', 'col')), may hold values from 0.5 to 4
- sketch_rows: int32 [32768], P(('row', 'col')), may hold values from 0 to 1023
- sketch_signs: int32 [32768], P(('row', 'col')), may hold values from 0 to 1
- right_side: float32 [16, 32768], P(None, ('row', 'col')), may hold values from -70 to 70
Outputs:
- solution: float32 [16, 32768], P(None, ('row', 'col'))
- last_basis: float32 [16, 32768], P(None, ('row', 'col'))
- hessenberg: float32 [16, 5, 4], replicated
The draws below stay inside these ranges and needn't reach their ends.
Inputs may be any that keep to these rules, and one draw needn't show every extreme that they name: `block_columns`: for block row b all 8 entries are distinct block columns c with (c - b) mod 128 <= 4 or >= 124; only slots k < tile_counts[b] are used. `tile_counts`: in every draw the 4 block rows of at least one device all have 8.
All inputs are finite; a program needn't handle non-finite values.
Results may differ from the reference program's by a relative error of at most 0.0053.
Values may be sent and summed in bfloat16 or wider, within the bound.
A program may use at most 64 MiB of HBM per device.

```python
import math
import jax
import jax.numpy as jnp
from jax import lax

TILE = 256
SKETCH = 1024
KMAX = 8
ITERS = 4
BR_DEV = 4
RHS = 16
NB = 128
N = 32768


def draw_block_columns(key, part):
    span = 2 * BR_DEV + 1
    scores = jax.random.randint(jax.random.fold_in(key, 11), (NB, span), 0, 1 << 20) * span + jnp.arange(span)[None, :]
    order = jnp.argsort(scores, axis=1, stable=True)
    offsets = order[:, :KMAX] - BR_DEV
    return ((jnp.arange(NB)[:, None] + offsets) % NB).astype(jnp.int32)


def draw_tile_counts(key, part):
    groups = NB // BR_DEV
    heavy = jax.random.randint(jax.random.fold_in(key, 21), (groups,), 0, 4) == 0
    forced = jnp.arange(groups) == jax.random.randint(jax.random.fold_in(key, 22), (), 0, groups)
    heavy = jnp.logical_or(heavy, forced)
    light = jax.random.randint(jax.random.fold_in(key, 23), (NB,), 1, KMAX // 2 + 1)
    return jnp.where(jnp.repeat(heavy, BR_DEV), KMAX, light).astype(jnp.int32)


def draw_right_side(key, part):
    scales = jnp.exp(jax.random.uniform(jax.random.fold_in(key, 31), (1, NB, 1), minval=0.0, maxval=math.log(10.0)))
    value = jax.random.truncated_normal(jax.random.fold_in(key, 32), -6.0, 6.0, (RHS, NB, TILE)) * scales
    return value.reshape(RHS, NB * TILE).astype(jnp.float32)


def with_ends(values, key, least, high):
    extent = values.shape
    index_at = [jax.random.randint(jax.random.fold_in(key, axis), (), 0, extent[axis]) for axis in range(len(extent))]
    values = values.at[tuple(index_at)].set(least)
    longest = extent.index(max(extent))
    index_at[longest] = (index_at[longest] + 1) % extent[longest]
    return values.at[tuple(index_at)].set(high)


def block_scale(rng, dims, pieces, low, high):
    level = 1.0
    for position, parts in pieces:
        draws = jax.random.uniform(jax.random.fold_in(jax.random.fold_in(rng, 6), position), (parts,), jnp.float32, low / len(pieces), high / len(pieces))
        level = level * jnp.repeat(jnp.exp(draws), dims[position] // parts).reshape((-1,) + (1,) * (len(dims) - 1 - position))
    return level


def noise(own_key, extent, spread, most, shards=(), dtype=jnp.bfloat16):
    values = spread * jax.random.normal(own_key, extent, jnp.float32)
    if shards:
        values = values * block_scale(own_key, extent, shards, -0.22, 0.18)
    return jnp.clip(values, -most, most).astype(dtype)


def setup_inputs(seed: int = 0) -> dict:
    key_of = jax.random.split(jax.random.key(seed), 8)
    return {
        "tile_values": noise(key_of[0], (NB, KMAX, TILE, TILE), TILE ** -0.5, 0.375, ((0, 32),)),
        "block_columns": draw_block_columns(jax.random.fold_in(key_of[7], 71), 0),
        "tile_counts": draw_tile_counts(jax.random.fold_in(key_of[7], 71), 0),
        "diagonal": jnp.clip(jnp.exp(math.log(4.0) - 2.0794415 * jax.random.uniform(key_of[3], (N,), jnp.float32) ** block_scale(key_of[3], (N,), ((0, 32),), -0.2, 0.2)), 0.5, 4.0),
        "sketch_rows": with_ends(jax.random.randint(key_of[4], (N,), 0, SKETCH), jax.random.fold_in(key_of[4], 1), 0, SKETCH - 1).astype(jnp.int32),
        "sketch_signs": with_ends(jax.random.randint(key_of[5], (N,), 0, 2), jax.random.fold_in(key_of[5], 1), 0, 1).astype(jnp.int32),
        "right_side": draw_right_side(jax.random.fold_in(key_of[7], 71), 0),
    }


epsilon = 1e-06
highest = lax.Precision.HIGHEST

def cholesky_solve(gram, target):
    order = gram.shape[1]
    factor = {}
    for column in range(order):
        diag_part = gram[:, column, column]
        for inner in range(column):
            diag_part = diag_part - factor[column, inner] * factor[column, inner]
        factor[column, column] = jnp.sqrt(diag_part)
        for below in range(column + 1, order):
            entry = gram[:, below, column]
            for inner in range(column):
                entry = entry - factor[below, inner] * factor[column, inner]
            factor[below, column] = entry / factor[column, column]
    forward = []
    for column in range(order):
        entry = target[:, column]
        for inner in range(column):
            entry = entry - factor[column, inner] * forward[inner]
        forward.append(entry / factor[column, column])
    result = [None] * order
    for column in reversed(range(order)):
        entry = forward[column]
        for inner in range(column + 1, order):
            entry = entry - factor[inner, column] * result[inner]
        result[column] = entry / factor[column, column]
    return jnp.stack(result, axis=1)

def sketch_solve(stacked, image_sketch):
    gram = jnp.einsum('rjk,rmk->rjm', stacked, stacked, precision=highest)
    target = jnp.einsum('rjk,rk->rj', stacked, image_sketch, precision=highest)
    return cholesky_solve(gram, target)

def sketch_of(vector, sketch_rows, sketch_signs):
    signed = vector * (2 * sketch_signs - 1).astype(jnp.float32)[None, :]
    summed = jax.ops.segment_sum(signed.T, sketch_rows, num_segments=SKETCH)
    return summed.T / math.sqrt(N)

def apply_matrix(vector, tile_values, block_columns, tile_counts, diagonal):
    blocks = vector.astype(jnp.bfloat16).reshape(RHS, NB, TILE)
    live_mask = (jnp.arange(KMAX)[None, :] < tile_counts[:, None]).astype(jnp.float32)

    def add_slot(slot_turn, running):
        slot_tiles = lax.dynamic_index_in_dim(tile_values, slot_turn, 1, keepdims=False).astype(jnp.float32)
        wanted = lax.dynamic_index_in_dim(block_columns, slot_turn, 1, keepdims=False)
        picked = jnp.take(blocks, wanted, axis=1).astype(jnp.float32)
        weight_mask = lax.dynamic_index_in_dim(live_mask, slot_turn, 1, keepdims=False)
        product = jnp.einsum('rbi,boi->rbo', picked, slot_tiles, precision=highest)
        return running + product * weight_mask[None, :, None]
    tile_sum = lax.fori_loop(0, KMAX, add_slot, jnp.zeros((RHS, NB, TILE), jnp.float32))
    return diagonal[None, :] * vector + tile_sum.reshape(RHS, N)

def reference(tile_values, block_columns, tile_counts, diagonal, sketch_rows, sketch_signs, right_side):
    start = sketch_of(right_side, sketch_rows, sketch_signs)
    beta = jnp.sqrt(lax.optimization_barrier(jnp.sum(start * start, axis=1)) + epsilon)
    basis = [right_side / beta[:, None]]
    sketched = [start / beta[:, None]]
    columns_list = []
    for step_index in range(ITERS):
        image = apply_matrix(basis[-1], tile_values, block_columns, tile_counts, diagonal)
        image_sketch = sketch_of(image, sketch_rows, sketch_signs)
        stacked = jnp.stack(sketched, axis=1)
        coeffs = sketch_solve(stacked, image_sketch)
        fresh = image - jnp.einsum('rj,rjn->rn', coeffs, jnp.stack(basis, axis=1), precision=highest)
        fresh_sketch = sketch_of(fresh, sketch_rows, sketch_signs)
        norm_new = jnp.sqrt(lax.optimization_barrier(jnp.sum(fresh_sketch * fresh_sketch, axis=1)) + epsilon)
        basis.append(fresh / norm_new[:, None])
        sketched.append(fresh_sketch / norm_new[:, None])
        padding = jnp.zeros((RHS, ITERS - step_index - 1), jnp.float32)
        columns_list.append(jnp.concatenate([coeffs, norm_new[:, None], padding], axis=1))
    hessenberg = jnp.stack(columns_list, axis=2)
    gram = jnp.einsum('rim,rin->rmn', hessenberg, hessenberg, precision=highest)
    weights = cholesky_solve(gram, beta[:, None] * hessenberg[:, 0, :])
    solution = jnp.einsum('rm,rmn->rn', weights, jnp.stack(basis[:ITERS], axis=1), precision=highest)
    return (solution, basis[-1], hessenberg)
```

```python
import functools
import math

import jax
import jax.numpy as jnp
from jax import lax
from jax.experimental import pallas as pl
from jax.experimental.pallas import tpu as pltpu
from jax.sharding import PartitionSpec as P

SKETCH = 1024
ITERS = 4
PARTS = 3
SHIFT = 1.75
epsilon = 1e-06
MESH = pl.DeviceIdType.MESH
f32 = jnp.float32
bf16 = jnp.bfloat16


def split_parts(value):
    parts = []
    for _ in range(PARTS - 1):
        head = value.astype(bf16)
        parts.append(head)
        value = value - head.astype(f32)
    parts.append(value.astype(bf16))
    return parts


def cholesky_solve(gram, target):
    order = len(target)
    factor = {}
    inverse = []
    for column in range(order):
        diag_part = gram[column, column]
        for inner in range(column):
            diag_part = diag_part - factor[column, inner] * factor[column, inner]
        inverse.append(1.0 / jnp.sqrt(diag_part))
        for below in range(column + 1, order):
            entry = gram[below, column]
            for inner in range(column):
                entry = entry - factor[below, inner] * factor[column, inner]
            factor[below, column] = entry * inverse[column]
    forward = []
    for column in range(order):
        entry = target[column]
        for inner in range(column):
            entry = entry - factor[column, inner] * forward[inner]
        forward.append(entry * inverse[column])
    result = [None] * order
    for column in reversed(range(order)):
        entry = forward[column]
        for inner in range(column + 1, order):
            entry = entry - factor[inner, column] * result[inner]
        result[column] = entry * inverse[column]
    return result


def inner_product(a, b):
    return jnp.sum(jnp.sum(a * b, axis=0), axis=1, keepdims=True)


def nt_dot(a, b):
    return lax.dot_general(a, b, (((1,), (1,)), ((), ())), preferred_element_type=f32)


def kernel(
    rows,
    cols,
    scaling,
    columns_ref,
    counts_ref,
    aux_ref,
    right_ref,
    tiles_hbm,
    solution_ref,
    last_ref,
    hess_ref,
    tiles,
    projector,
    krylov,
    window,
    index_ref,
    halo,
    part,
    land1,
    land2,
    sketches,
    tile_sem,
    halo_send,
    halo_recv,
    send1,
    recv1,
    send2,
    recv2,
    send3,
    recv3,
):
    row = lax.axis_index("row")
    col = lax.axis_index("col")
    devices = rows * cols
    me = row * cols + col
    block_rows, slots, tile, _ = tiles.shape
    systems, width = right_ref.shape
    all_blocks = block_rows * devices
    share = SKETCH // cols
    right = lax.rem(me + 1, devices)
    left = lax.rem(me + devices - 1, devices)
    right = (lax.div(right, cols), lax.rem(right, cols))
    left = (lax.div(left, cols), lax.rem(left, cols))
    col_to = [lax.rem(col + off, cols) for off in range(cols)]
    col_from = [lax.rem(col + cols - off, cols) for off in range(cols)]
    row_to = [lax.rem(row + off, rows) for off in range(rows)]
    row_from = [lax.rem(row + rows - off, rows) for off in range(rows)]

    barrier = pltpu.get_barrier_semaphore()
    for peer in (left, right):
        pl.semaphore_signal(barrier, inc=1, device_id=peer, device_id_type=MESH)
    for off in range(1, rows):
        pl.semaphore_signal(barrier, inc=1, device_id=(row_to[off], col), device_id_type=MESH)
    for off in range(1, cols):
        pl.semaphore_signal(barrier, inc=1, device_id=(row, col_to[off]), device_id_type=MESH)

    tile_copy = pltpu.make_async_copy(tiles_hbm, tiles, tile_sem)
    tile_copy.start()

    first = me * block_rows
    for b in range(block_rows):
        for slot in range(slots):
            spot = lax.rem(columns_ref[b, slot] - first + block_rows + all_blocks, all_blocks)
            index_ref[b * slots + slot] = jnp.where(slot < counts_ref[b], spot, 3 * block_rows)
    window[3 * block_rows] = jnp.zeros(window.shape[1:], window.dtype)

    pl.semaphore_wait(barrier, rows + cols)

    def halo_copies(k):
        source = right_ref if k == 0 else krylov.at[k]
        return [
            pltpu.make_async_remote_copy(
                src_ref=source,
                dst_ref=halo.at[k, side],
                send_sem=halo_send.at[k, side],
                recv_sem=halo_recv.at[k, side],
                device_id=peer,
                device_id_type=MESH,
            )
            for side, peer in ((0, right), (1, left))
        ]

    def copy1(k, off, block):
        return pltpu.make_async_remote_copy(
            src_ref=part.at[k, block],
            dst_ref=land1.at[k, off - 1],
            send_sem=send1.at[k, off - 1],
            recv_sem=recv1.at[k, off - 1],
            device_id=(row, col_to[off]),
            device_id_type=MESH,
        )

    def copy2(k, off, source):
        return pltpu.make_async_remote_copy(
            src_ref=land2.at[k, source],
            dst_ref=land2.at[k, source],
            send_sem=send2.at[k, off - 1],
            recv_sem=recv2.at[k, off - 1],
            device_id=(row_to[off], col),
            device_id_type=MESH,
        )

    def copy3(k, off, source):
        return pltpu.make_async_remote_copy(
            src_ref=sketches.at[k, source],
            dst_ref=sketches.at[k, source],
            send_sem=send3.at[k, off - 1],
            recv_sem=recv3.at[k, off - 1],
            device_id=(row, col_to[off]),
            device_id_type=MESH,
        )

    def place(value, base):
        parts = split_parts(value)
        for b in range(block_rows):
            piece = [p[:, b * tile : (b + 1) * tile] for p in parts]
            window[base + b] = jnp.concatenate(piece, axis=0)

    def stage1(k):
        for block in range(cols):
            total = None
            for b in range(block_rows):
                term = nt_dot(
                    window[block_rows + b],
                    projector[pl.ds(block * share, share), pl.ds(b * tile, tile)],
                )
                total = term if total is None else total + term
            summed = total[(PARTS - 1) * systems :]
            for p in reversed(range(PARTS - 1)):
                summed = summed + total[p * systems : (p + 1) * systems]
            part[k, block] = summed * scaling
        for off in range(1, cols):
            copy1(k, off, col_to[off]).start()

    def stage2(k):
        for off in range(1, cols):
            copy1(k, off, 0).wait_recv()
        total = part[k, col]
        for off in range(1, cols):
            total = total + land1[k, off - 1]
        land2[k, row] = total
        for off in range(1, rows):
            copy2(k, off, row).start()

    def stage3(k):
        for off in range(1, rows):
            copy2(k, off, row_from[off]).wait_recv()
        total = land2[k, 0]
        for r in range(1, rows):
            total = total + land2[k, r]
        sketches[k, col] = total
        for off in range(1, cols):
            copy3(k, off, col).start()

    def finish(k):
        for off in range(1, cols):
            copy3(k, off, col_from[off]).wait_recv()

    for k in range(ITERS + 1):
        if k == 0:
            for copy in halo_copies(0):
                copy.start()
            krylov[0] = right_ref[...]
            diag = aux_ref[0:1, :] - SHIFT
            signed = aux_ref[1:2, :]
            targets = aux_ref[2:3, :].astype(jnp.int32)
            chunk = 64

            def build(step, carry):
                base = pl.multiple_of(step * chunk, chunk)
                spots = lax.broadcasted_iota(jnp.int32, (chunk, width), 0) + base
                projector[pl.ds(base, chunk), :] = jnp.where(
                    spots == targets, signed, 0.0
                ).astype(bf16)
                return carry

            lax.fori_loop(0, SKETCH // chunk, build, 0)
            place(right_ref[...], block_rows)
        stage1(k)
        if k >= 1:
            stage2(k - 1)
        if k >= 2:
            stage3(k - 2)
        if k == ITERS:
            break
        for copy in halo_copies(k):
            copy.wait_recv()
        place(halo[k, 0], 0)
        place(halo[k, 1], 2 * block_rows)
        if k == 0:
            tile_copy.wait()
        for b in range(block_rows):
            total = None
            for slot in range(slots):
                term = nt_dot(window[index_ref[b * slots + slot]], tiles[b, slot])
                total = term if total is None else total + term
            summed = total[(PARTS - 1) * systems :]
            for p in reversed(range(PARTS - 1)):
                summed = summed + total[p * systems : (p + 1) * systems]
            lanes = pl.ds(b * tile, tile)
            diag_b = aux_ref[0:1, lanes] - SHIFT
            krylov[k + 1, :, lanes] = diag_b * krylov[k, :, lanes] + summed
        if k + 1 < ITERS:
            for copy in halo_copies(k + 1):
                copy.start()
        place(krylov[k + 1], block_rows)

    coords = []
    sketched = []
    gram = {}
    hess = {}

    def arnoldi(j):
        spread = [None] * (j + 1)
        for i in range(j):
            spread[i] = SHIFT * coords[j - 1][i]
        for i in range(j):
            moved = coords[j - 1][i]
            spread[i + 1] = moved if spread[i + 1] is None else spread[i + 1] + moved
        image = spread[0] * sketches[0]
        for i in range(1, j + 1):
            image = image + spread[i] * sketches[i]
        target = [inner_product(q, image) for q in sketched]
        coeffs = cholesky_solve(gram, target)
        for i in range(j):
            image = image - coeffs[i] * sketched[i]
            for m in range(i + 1):
                spread[m] = spread[m] - coeffs[i] * coords[i][m]
        square = inner_product(image, image) + epsilon
        norm = jnp.sqrt(square)
        scale = 1.0 / norm
        for i in range(j):
            hess[i, j - 1] = coeffs[i]
        hess[j, j - 1] = norm
        coords.append([entry * scale for entry in spread])
        if j < ITERS:
            add_sketched(image * scale)

    def add_sketched(q):
        sketched.append(q)
        n = len(sketched)
        for i in range(n):
            gram[n - 1, i] = inner_product(q, sketched[i])

    finish(0)
    start = sketches[0]
    beta = jnp.sqrt(inner_product(start, start) + epsilon)
    coords.append([1.0 / beta])
    add_sketched(start * coords[0][0])
    finish(1)
    arnoldi(1)
    stage2(ITERS)
    stage3(ITERS - 1)
    finish(2)
    arnoldi(2)
    stage3(ITERS)
    finish(3)
    arnoldi(3)
    finish(4)
    arnoldi(4)

    lane = lax.broadcasted_iota(jnp.int32, hess_ref.shape, 1)
    packed = jnp.zeros(hess_ref.shape, f32)
    for (i, j), value in hess.items():
        packed = jnp.where(lane == i * ITERS + j, value, packed)
    hess_ref[...] = packed

    normal = {}
    for m in range(ITERS):
        for n in range(m + 1):
            entry = None
            for i in range(min(m, n) + 2):
                term = hess[i, m] * hess[i, n]
                entry = term if entry is None else entry + term
            normal[m, n] = entry
    weights = cholesky_solve(normal, [beta * hess[0, n] for n in range(ITERS)])
    mixed = []
    for m in range(ITERS):
        entry = None
        for i in range(m, ITERS):
            term = weights[i] * coords[i][m]
            entry = term if entry is None else entry + term
        mixed.append(entry)
    out = mixed[0] * krylov[0]
    for m in range(1, ITERS):
        out = out + mixed[m] * krylov[m]
    solution_ref[...] = out
    out = coords[ITERS][0] * krylov[0]
    for m in range(1, ITERS + 1):
        out = out + coords[ITERS][m] * krylov[m]
    last_ref[...] = out

    for k in range(ITERS + 1):
        if k < ITERS:
            for copy in halo_copies(k):
                copy.wait_send()
        for off in range(1, cols):
            copy1(k, off, col_to[off]).wait_send()
            copy3(k, off, col).wait_send()
        for off in range(1, rows):
            copy2(k, off, row).wait_send()


def local(
    rows, cols, tile_values, block_columns, tile_counts, diagonal, sketch_rows, sketch_signs, right_side
):
    block_rows, _, tile, _ = tile_values.shape
    systems, width = right_side.shape
    scaling = 1.0 / math.sqrt(width * rows * cols)
    share = SKETCH // cols
    vectors = ITERS + 1
    aux = jnp.stack(
        [diagonal, (2 * sketch_signs - 1).astype(f32), sketch_rows.astype(f32)], axis=0
    )
    vmem = pl.BlockSpec(memory_space=pltpu.VMEM)
    smem = pl.BlockSpec(memory_space=pltpu.SMEM)
    dma = pltpu.SemaphoreType.DMA
    iterate, last, packed = pl.pallas_call(
        functools.partial(kernel, rows, cols, scaling),
        out_shape=(
            jax.ShapeDtypeStruct((systems, width), f32),
            jax.ShapeDtypeStruct((systems, width), f32),
            jax.ShapeDtypeStruct((systems, 128), f32),
        ),
        in_specs=[smem, smem, vmem, vmem, pl.BlockSpec(memory_space=pl.ANY)],
        out_specs=(vmem, vmem, vmem),
        scratch_shapes=[
            pltpu.VMEM(tile_values.shape, bf16),
            pltpu.VMEM((SKETCH, width), bf16),
            pltpu.VMEM((vectors, systems, width), f32),
            pltpu.VMEM((3 * block_rows + 1, PARTS * systems, tile), bf16),
            pltpu.SMEM((tile_values.shape[0] * tile_values.shape[1],), jnp.int32),
            pltpu.VMEM((ITERS, 2, systems, width), f32),
            pltpu.VMEM((vectors, cols, systems, share), f32),
            pltpu.VMEM((vectors, cols - 1, systems, share), f32),
            pltpu.VMEM((vectors, rows, systems, share), f32),
            pltpu.VMEM((vectors, cols, systems, share), f32),
            dma,
            dma((ITERS, 2)),
            dma((ITERS, 2)),
            dma((vectors, cols - 1)),
            dma((vectors, cols - 1)),
            dma((vectors, rows - 1)),
            dma((vectors, rows - 1)),
            dma((vectors, cols - 1)),
            dma((vectors, cols - 1)),
        ],
        compiler_params=pltpu.CompilerParams(
            collective_id=0, has_side_effects=True, vmem_limit_bytes=48 * 1024 * 1024
        ),
    )(block_columns, tile_counts, aux, right_side, tile_values)
    hessenberg = packed[:, : (ITERS + 1) * ITERS].reshape(systems, ITERS + 1, ITERS)
    return iterate, last, hessenberg


def solution(mesh):
    spec = P(("row", "col"))
    in_specs = (
        P(("row", "col"), None, None, None),
        P(("row", "col"), None),
        spec,
        spec,
        spec,
        spec,
        P(None, ("row", "col")),
    )
    out_specs = (P(None, ("row", "col")), P(None, ("row", "col")), P())
    body = functools.partial(local, mesh.shape["row"], mesh.shape["col"])
    return jax.shard_map(body, mesh=mesh, in_specs=in_specs, out_specs=out_specs, check_vma=False)
```

```python
import functools
import math

import jax
import jax.numpy as jnp
from jax import lax
from jax.experimental import pallas as pl
from jax.experimental.pallas import tpu as pltpu
from jax.sharding import PartitionSpec as P

SKETCH = 1024
ITERS = 4
PARTS = 3
SHIFT = 1.75
epsilon = 1e-06
MESH = pl.DeviceIdType.MESH
f32 = jnp.float32
bf16 = jnp.bfloat16


def split_parts(value):
    parts = []
    for _ in range(PARTS - 1):
        head = value.astype(bf16)
        parts.append(head)
        value = value - head.astype(f32)
    parts.append(value.astype(bf16))
    return parts


def extend_factor(factor, inverse, entries):
    row = len(inverse)
    for column in range(row):
        entry = entries[column]
        for inner in range(column):
            entry = entry - factor[row, inner] * factor[column, inner]
        factor[row, column] = entry * inverse[column]
    diag_part = entries[row]
    for inner in range(row):
        diag_part = diag_part - factor[row, inner] * factor[row, inner]
    inverse.append(1.0 / jnp.sqrt(diag_part))


def factor_solve(factor, inverse, target):
    order = len(target)
    forward = []
    for column in range(order):
        entry = target[column]
        for inner in range(column):
            entry = entry - factor[column, inner] * forward[inner]
        forward.append(entry * inverse[column])
    result = [None] * order
    for column in reversed(range(order)):
        entry = forward[column]
        for inner in range(column + 1, order):
            entry = entry - factor[inner, column] * result[inner]
        result[column] = entry * inverse[column]
    return result


def inner_product(a, b):
    return jnp.sum(jnp.sum(a * b, axis=0), axis=1, keepdims=True)


def nt_dot(a, b):
    return lax.dot_general(a, b, (((1,), (1,)), ((), ())), preferred_element_type=f32)


def kernel(
    rows,
    cols,
    scaling,
    columns_hbm,
    counts_hbm,
    diag_hbm,
    rows_hbm,
    signs_hbm,
    right_hbm,
    tiles_hbm,
    solution_ref,
    last_ref,
    hess_ref,
    columns_ref,
    counts_ref,
    diag_ref,
    rows_ref,
    signs_ref,
    tiles,
    projector,
    krylov,
    window,
    index_ref,
    halo,
    part,
    land1,
    land2,
    sketches,
    load_sem,
    halo_send,
    halo_recv,
    send1,
    recv1,
    send2,
    recv2,
    send3,
    recv3,
):
    row = lax.axis_index("row")
    col = lax.axis_index("col")
    devices = rows * cols
    me = row * cols + col
    block_rows, slots, tile, _ = tiles.shape
    systems, width = right_hbm.shape
    all_blocks = block_rows * devices
    share = SKETCH // cols
    right = lax.rem(me + 1, devices)
    left = lax.rem(me + devices - 1, devices)
    right = (lax.div(right, cols), lax.rem(right, cols))
    left = (lax.div(left, cols), lax.rem(left, cols))
    col_to = [lax.rem(col + off, cols) for off in range(cols)]
    col_from = [lax.rem(col + cols - off, cols) for off in range(cols)]
    row_to = [lax.rem(row + off, rows) for off in range(rows)]
    row_from = [lax.rem(row + rows - off, rows) for off in range(rows)]

    barrier = pltpu.get_barrier_semaphore()
    for peer in (left, right):
        pl.semaphore_signal(barrier, inc=1, device_id=peer, device_id_type=MESH)
    for off in range(1, rows):
        pl.semaphore_signal(barrier, inc=1, device_id=(row_to[off], col), device_id_type=MESH)
    for off in range(1, cols):
        pl.semaphore_signal(barrier, inc=1, device_id=(row, col_to[off]), device_id_type=MESH)

    loads = [
        pltpu.make_async_copy(source, target, load_sem.at[n])
        for n, (source, target) in enumerate(
            [
                (rows_hbm, rows_ref),
                (signs_hbm, signs_ref),
                (columns_hbm, columns_ref),
                (counts_hbm, counts_ref),
                (diag_hbm, diag_ref),
            ]
            + [
                (right_hbm.at[:, pl.ds(b * tile, tile)], krylov.at[0, b])
                for b in range(block_rows)
            ]
            + [(tiles_hbm, tiles)]
        )
    ]
    for load in loads:
        load.start()
    for load in loads[:4]:
        load.wait()

    first = me * block_rows
    for b in range(block_rows):
        for slot in range(slots):
            spot = lax.rem(columns_ref[b, slot] - first + block_rows + all_blocks, all_blocks)
            index_ref[b * slots + slot] = jnp.where(slot < counts_ref[b], spot, 3 * block_rows)
    window[3 * block_rows] = jnp.zeros(window.shape[1:], window.dtype)

    signed = (2 * signs_ref[...] - 1).astype(f32)
    targets = rows_ref[...]
    chunk = 64

    def build(step, carry):
        base = pl.multiple_of(step * chunk, chunk)
        spots = lax.broadcasted_iota(jnp.int32, (chunk, width), 0) + base
        projector[pl.ds(base, chunk), :] = jnp.where(spots == targets, signed, 0.0).astype(bf16)
        return carry

    lax.fori_loop(0, SKETCH // chunk, build, 0)
    for load in loads[4:-1]:
        load.wait()
    pl.semaphore_wait(barrier, rows + cols)

    def halo_copies(k, b):
        return [
            pltpu.make_async_remote_copy(
                src_ref=krylov.at[k, b],
                dst_ref=halo.at[k, side, b],
                send_sem=halo_send.at[k, side, b],
                recv_sem=halo_recv.at[k, side, b],
                device_id=peer,
                device_id_type=MESH,
            )
            for side, peer in ((0, right), (1, left))
        ]

    def copy1(k, off, block):
        return pltpu.make_async_remote_copy(
            src_ref=part.at[k, block],
            dst_ref=land1.at[k, off - 1],
            send_sem=send1.at[k, off - 1],
            recv_sem=recv1.at[k, off - 1],
            device_id=(row, col_to[off]),
            device_id_type=MESH,
        )

    def copy2(k, off, source):
        return pltpu.make_async_remote_copy(
            src_ref=land2.at[k, source],
            dst_ref=land2.at[k, source],
            send_sem=send2.at[k, off - 1],
            recv_sem=recv2.at[k, off - 1],
            device_id=(row_to[off], col),
            device_id_type=MESH,
        )

    def copy3(k, off, source):
        return pltpu.make_async_remote_copy(
            src_ref=sketches.at[k, source],
            dst_ref=sketches.at[k, source],
            send_sem=send3.at[k, off - 1],
            recv_sem=recv3.at[k, off - 1],
            device_id=(row, col_to[off]),
            device_id_type=MESH,
        )

    def place(value, spot):
        window[spot] = jnp.concatenate(split_parts(value), axis=0)

    def stage1(k):
        for block in range(cols):
            total = None
            for b in range(block_rows):
                term = nt_dot(
                    window[block_rows + b],
                    projector[pl.ds(block * share, share), pl.ds(b * tile, tile)],
                )
                total = term if total is None else total + term
            summed = total[(PARTS - 1) * systems :]
            for p in reversed(range(PARTS - 1)):
                summed = summed + total[p * systems : (p + 1) * systems]
            part[k, block] = summed * scaling
        for off in range(1, cols):
            copy1(k, off, col_to[off]).start()

    def stage2(k):
        for off in range(1, cols):
            copy1(k, off, 0).wait_recv()
        total = part[k, col]
        for off in range(1, cols):
            total = total + land1[k, off - 1]
        land2[k, row] = total
        for off in range(1, rows):
            copy2(k, off, row).start()

    def stage3(k):
        for off in range(1, rows):
            copy2(k, off, row_from[off]).wait_recv()
        total = land2[k, 0]
        for r in range(1, rows):
            total = total + land2[k, r]
        sketches[k, col] = total
        for off in range(1, cols):
            copy3(k, off, col).start()

    def finish(k):
        for off in range(1, cols):
            copy3(k, off, col_from[off]).wait_recv()

    coords = []
    sketched = []
    factor, inverse = {}, []
    hess = {}
    normal, normal_inverse = {}, []

    def spread_of(j):
        spread = [SHIFT * entry for entry in coords[j - 1]] + [None]
        for i in range(j):
            moved = coords[j - 1][i]
            spread[i + 1] = moved if spread[i + 1] is None else spread[i + 1] + moved
        image = spread[0] * sketches[0]
        for i in range(1, j):
            image = image + spread[i] * sketches[i]
        return spread, image

    def arnoldi(j, prepared):
        spread, image = prepared
        image = image + spread[j] * sketches[j]
        coeffs = factor_solve(factor, inverse, [inner_product(q, image) for q in sketched])
        for i in range(j):
            image = image - coeffs[i] * sketched[i]
            for m in range(i + 1):
                spread[m] = spread[m] - coeffs[i] * coords[i][m]
        norm = jnp.sqrt(inner_product(image, image) + epsilon)
        scale = 1.0 / norm
        for i in range(j):
            hess[i, j - 1] = coeffs[i]
        hess[j, j - 1] = norm
        coords.append([entry * scale for entry in spread])
        if j < ITERS:
            add_sketched(image * scale)
        entries = []
        for n in range(j):
            entry = None
            for i in range(n + 2):
                term = hess[i, j - 1] * hess[i, n]
                entry = term if entry is None else entry + term
            entries.append(entry)
        extend_factor(normal, normal_inverse, entries)

    def add_sketched(q):
        sketched.append(q)
        extend_factor(factor, inverse, [inner_product(q, other) for other in sketched])

    for b in range(block_rows):
        for copy in halo_copies(0, b):
            copy.start()
    for b in range(block_rows):
        place(krylov[0, b], block_rows + b)
    beta = None
    for k in range(ITERS):
        stage1(k)
        if k >= 1:
            stage3(k - 1)
        if k == 2:
            finish(0)
            start = sketches[0]
            beta = jnp.sqrt(inner_product(start, start) + epsilon)
            coords.append([1.0 / beta])
            add_sketched(start * coords[0][0])
        if k >= 3:
            finish(k - 2)
            arnoldi(k - 2, spread_of(k - 2))
        stage2(k)
        for b in range(block_rows):
            for copy in halo_copies(k, b):
                copy.wait_recv()
            place(halo[k, 0, b], b)
            place(halo[k, 1, b], 2 * block_rows + b)
        if k == 0:
            loads[-1].wait()
        for b in range(block_rows):
            total = None
            for slot in range(slots):
                term = nt_dot(window[index_ref[b * slots + slot]], tiles[b, slot])
                total = term if total is None else total + term
            summed = total[(PARTS - 1) * systems :]
            for p in reversed(range(PARTS - 1)):
                summed = summed + total[p * systems : (p + 1) * systems]
            diag_b = diag_ref[0:1, pl.ds(b * tile, tile)] - SHIFT
            krylov[k + 1, b] = diag_b * krylov[k, b] + summed
            if k + 1 < ITERS:
                for copy in halo_copies(k + 1, b):
                    copy.start()
        for b in range(block_rows):
            place(krylov[k + 1, b], block_rows + b)
    stage1(ITERS)
    stage3(ITERS - 1)
    finish(ITERS - 2)
    arnoldi(ITERS - 2, spread_of(ITERS - 2))
    stage2(ITERS)
    finish(ITERS - 1)
    arnoldi(ITERS - 1, spread_of(ITERS - 1))
    prepared = spread_of(ITERS)
    stage3(ITERS)
    finish(ITERS)
    arnoldi(ITERS, prepared)

    lane = lax.broadcasted_iota(jnp.int32, (systems, 128), 1)
    packed = jnp.zeros((systems, 128), f32)
    for (i, j), value in hess.items():
        packed = jnp.where(lane == i * ITERS + j, value, packed)
    turned = packed.T
    for i in range(ITERS + 1):
        hess_ref[i] = turned[i * ITERS : (i + 1) * ITERS, :]

    weights = factor_solve(normal, normal_inverse, [beta * hess[0, n] for n in range(ITERS)])
    mixed = []
    for m in range(ITERS):
        entry = None
        for i in range(m, ITERS):
            term = weights[i] * coords[i][m]
            entry = term if entry is None else entry + term
        mixed.append(entry)
    for b in range(block_rows):
        lanes = pl.ds(b * tile, tile)
        out = mixed[0] * krylov[0, b]
        for m in range(1, ITERS):
            out = out + mixed[m] * krylov[m, b]
        solution_ref[:, lanes] = out
        out = coords[ITERS][0] * krylov[0, b]
        for m in range(1, ITERS + 1):
            out = out + coords[ITERS][m] * krylov[m, b]
        last_ref[:, lanes] = out

    for k in range(ITERS + 1):
        if k < ITERS:
            for b in range(block_rows):
                for copy in halo_copies(k, b):
                    copy.wait_send()
        for off in range(1, cols):
            copy1(k, off, col_to[off]).wait_send()
            copy3(k, off, col).wait_send()
        for off in range(1, rows):
            copy2(k, off, row).wait_send()


def local(
    rows, cols, tile_values, block_columns, tile_counts, diagonal, sketch_rows, sketch_signs, right_side
):
    block_rows, _, tile, _ = tile_values.shape
    systems, width = right_side.shape
    scaling = 1.0 / math.sqrt(width * rows * cols)
    share = SKETCH // cols
    vectors = ITERS + 1
    vmem = pl.BlockSpec(memory_space=pltpu.VMEM)
    hbm = pl.BlockSpec(memory_space=pltpu.HBM)
    dma = pltpu.SemaphoreType.DMA
    iterate, last, hessenberg = pl.pallas_call(
        functools.partial(kernel, rows, cols, scaling),
        out_shape=(
            pltpu.VMEM((systems, width), f32),
            pltpu.VMEM((systems, width), f32),
            pltpu.VMEM((ITERS + 1, ITERS, systems), f32),
        ),
        in_specs=[hbm] * 7,
        out_specs=(vmem, vmem, vmem),
        scratch_shapes=[
            pltpu.SMEM(block_columns.shape, jnp.int32),
            pltpu.SMEM(tile_counts.shape, jnp.int32),
            pltpu.VMEM((1, width), f32),
            pltpu.VMEM((1, width), jnp.int32),
            pltpu.VMEM((1, width), jnp.int32),
            pltpu.VMEM(tile_values.shape, bf16),
            pltpu.VMEM((SKETCH, width), bf16),
            pltpu.VMEM((vectors, block_rows, systems, tile), f32),
            pltpu.VMEM((3 * block_rows + 1, PARTS * systems, tile), bf16),
            pltpu.SMEM((tile_values.shape[0] * tile_values.shape[1],), jnp.int32),
            pltpu.VMEM((ITERS, 2, block_rows, systems, tile), f32),
            pltpu.VMEM((vectors, cols, systems, share), f32),
            pltpu.VMEM((vectors, cols - 1, systems, share), f32),
            pltpu.VMEM((vectors, rows, systems, share), f32),
            pltpu.VMEM((vectors, cols, systems, share), f32),
            dma((block_rows + 6,)),
            dma((ITERS, 2, block_rows)),
            dma((ITERS, 2, block_rows)),
            dma((vectors, cols - 1)),
            dma((vectors, cols - 1)),
            dma((vectors, rows - 1)),
            dma((vectors, rows - 1)),
            dma((vectors, cols - 1)),
            dma((vectors, cols - 1)),
        ],
        compiler_params=pltpu.CompilerParams(
            collective_id=0, has_side_effects=True, vmem_limit_bytes=67043328 - 160 * 1024
        ),
    )(
        block_columns,
        tile_counts,
        diagonal.reshape(1, width),
        sketch_rows.reshape(1, width),
        sketch_signs.reshape(1, width),
        right_side,
        tile_values,
    )
    return iterate, last, jnp.transpose(hessenberg, (2, 0, 1))


def solution(mesh):
    spec = P(("row", "col"))
    in_specs = (
        P(("row", "col"), None, None, None),
        P(("row", "col"), None),
        spec,
        spec,
        spec,
        spec,
        P(None, ("row", "col")),
    )
    out_specs = (P(None, ("row", "col")), P(None, ("row", "col")), P())
    body = functools.partial(local, mesh.shape["row"], mesh.shape["col"])
    return jax.shard_map(body, mesh=mesh, in_specs=in_specs, out_specs=out_specs, check_vma=False)
```
